256 devices in a mesh: row: 8 (over x, core), col: 32 (over z, y).
Axes of the slice: x: 4, y: 4, z: 8, core: 2. Of those that a mesh axis runs over, the one named last changes fastest.
Arguments:
- diag_block: float32 [512, 512], P(None, 'col'), may hold values from -0.2 to 2, as said below
- panel_below: float32 [16384, 512], P('col', 'row'), may hold values from -0.26516503 to 0.26516503
- trail_inverse: float32 [16384, 16384], P('row', 'col'), may hold values from -0.046875 to 0.046875
Outputs:
- inverse_panel: float32 [16384, 512], P('row', 'col')
- product_panel: float32 [16384, 512], P('col', 'row')
The draws below stay inside these ranges and needn't reach their ends.
Inputs may be any that keep to these rules, and one draw needn't show every extreme that they name: diag_block is lower triangular with diagonal entries between 1 and 2 and off-diagonal entries of magnitude at most 0.2.
All inputs are finite; a program needn't handle non-finite values.
Results may differ from the reference program's by a relative error of at most 0.000094.
Values sent between devices are 32-bit elements; how exact they have to be, the bound alone decides.
No kernel may reach another device: no remote copies, remote signals or barrier semaphores. Data moves between devices by JAX's collectives and lax.ppermute only.
A program may use at most 64 MiB of HBM per device.

```python
import jax
import jax.numpy as jnp
from jax import lax

BLOCK = 512
M = 16384
CYC = 512
N_ROW = 8
N_COL = 32


def draw_diag_block(key, part):
    first, second = jax.random.split(jax.random.fold_in(key, 11))
    lower = jnp.clip(jax.random.normal(first, (BLOCK, BLOCK), jnp.float32) * (0.5 / BLOCK ** 0.5), -0.2, 0.2)
    diagonal = jax.random.uniform(second, (BLOCK,), jnp.float32, 1.0, 2.0)
    return jnp.tril(lower, -1) + jnp.diag(diagonal)


def shard_levels(stream_key, dims, shards, least, top_value):
    def one(dim, shards_of):
        heights = jax.random.uniform(jax.random.fold_in(jax.random.fold_in(stream_key, 6), dim), (shards_of,), jnp.float32, least / len(shards), top_value / len(shards))
        return jnp.repeat(jnp.exp(heights), dims[dim] // shards_of).reshape((-1,) + (1,) * (len(dims) - dim - 1))

    gain = one(*shards[0])
    for cut in shards[1:]:
        gain = gain * one(*cut)
    return gain


def scatter_about(key, extent, deviation, reach, cuts=(), kind=jnp.bfloat16):
    gain = shard_levels(key, extent, cuts, -0.22, 0.18) if cuts else 1.0
    drawn = jax.random.normal(key, extent, jnp.float32) * deviation * gain
    return jnp.minimum(jnp.maximum(drawn, -reach), reach).astype(kind)


def setup_inputs(seed: int = 0) -> dict:
    key_of = jax.random.split(jax.random.key(seed), 4)
    diag_block = draw_diag_block(jax.random.fold_in(key_of[3], 71), 0)
    panel_below = scatter_about(key_of[1], (M, BLOCK), (BLOCK ** -0.5), 0.26516503, ((0, 32), (1, 8)), jnp.float32)
    trail_inverse = scatter_about(key_of[2], (M, M), M ** -0.5, 0.046875, ((0, 8), (1, 32)), jnp.float32)
    return dict(diag_block=diag_block, panel_below=panel_below, trail_inverse=trail_inverse)


def storage_map(count, parts):
    position = jnp.arange(M, dtype=jnp.int32)
    per_part = M // parts
    owner = position // per_part
    local = position % per_part
    return (local // CYC * parts + owner) * CYC + local % CYC

def reference(diag_block, panel_below, trail_inverse):
    high = lax.Precision.HIGHEST
    eye_block = jnp.eye(BLOCK, dtype=jnp.float32)
    inverse_block = jax.scipy.linalg.solve_triangular(diag_block, eye_block, lower=True)
    scaled = jnp.dot(panel_below.astype(jnp.float32), inverse_block.astype(jnp.float32), precision=high, preferred_element_type=jnp.float32)
    rowmap = storage_map(M, N_ROW)
    colmap = storage_map(M, N_COL)
    below = rowmap[:, None] >= colmap[None, :]
    same = rowmap[:, None] == colmap[None, :]
    factor = jnp.where(below, trail_inverse, jnp.float32(0.0)) + jnp.where(same, jnp.float32(1.0), jnp.float32(0.0))
    inverse_panel = -jnp.dot(factor.astype(jnp.float32), scaled.astype(jnp.float32), precision=high, preferred_element_type=jnp.float32)
    product_panel = lax.dot_general(factor.astype(jnp.float32), inverse_panel.astype(jnp.float32), (((0,), (0,)), ((), ())), precision=high, preferred_element_type=jnp.float32)
    return (inverse_panel, product_panel)
```

```python
import functools

import jax
import jax.numpy as jnp
from jax import lax
from jax.experimental import pallas as pl
from jax.experimental.pallas import tpu as pltpu
from jax.sharding import Mesh
from jax.sharding import PartitionSpec as P


ROW = ("x", "core")
COL = ("z", "y")
NX, NC, NZ, NY = 4, 2, 8, 4
NR, NCOL = NX * NC, NZ * NY
BLK = 512
ROWS = 2048
R1 = 48
R2 = 64 - R1
H1 = NZ * R1
H2 = NY * R2
BASE2 = NCOL * R1

OFF1 = {2: 0, 1: H1 + H2, 3: 2 * H1 + H2, 0: 3 * H1 + H2}
OFF2 = {4: H1}
for place, hop in enumerate((3, 5, 2, 6, 1, 7, 0)):
    OFF2[hop] = 4 * H1 + (place + 1) * H2
FIRST = H1 + H2

VMEM = pl.BlockSpec(memory_space=pltpu.VMEM)
SMEM = pl.BlockSpec(memory_space=pltpu.SMEM)
NT = (((1,), (1,)), ((), ()))
TN = (((0,), (0,)), ((), ()))
NN = (((1,), (0,)), ((), ()))


def call(kernel, out, n_in, flops=0, scratch=(), smem=True):
    many = isinstance(out, (list, tuple))
    return pl.pallas_call(
        kernel,
        out_shape=out,
        in_specs=([SMEM] if smem else []) + [VMEM] * n_in,
        out_specs=[VMEM] * len(out) if many else VMEM,
        scratch_shapes=list(scratch),
        cost_estimate=pl.CostEstimate(flops=flops, bytes_accessed=1 << 20, transcendentals=0),
    )


def halves(value):
    high = value.astype(jnp.bfloat16)
    low = (value - high.astype(jnp.float32)).astype(jnp.bfloat16)
    return high, low


def dot(a, b, dims):
    return lax.dot_general(a, b, dims, preferred_element_type=jnp.float32)


def dot3(a, b, dims):
    return dot(a[0], b[0], dims) + (dot(a[0], b[1], dims) + dot(a[1], b[0], dims))


def dot_full(a, b, dims=NN):
    return lax.dot_general(
        a, b, dims, precision=lax.Precision.HIGHEST, preferred_element_type=jnp.float32
    )


def prepare_kernel(idx, w, high, low):
    x, core, z, y = idx[0], idx[1], idx[2], idx[3]
    shift = (x * NC + core) - (z * NY + y)

    def piece(source, target, size):
        source = pl.multiple_of(source, 8)
        target = pl.multiple_of(target, 16)
        row = lax.broadcasted_iota(jnp.int32, (size, 1), 0) + source
        place = ((row >> 9) * NR + shift) * BLK + (row & (BLK - 1))
        delta = place - lax.broadcasted_iota(jnp.int32, (size, BLK), 1)
        value = jnp.where(delta >= 0, w[pl.ds(source, size), :], 0.0) + jnp.where(
            delta == 0, 1.0, 0.0
        )
        a, b = halves(value)
        high[pl.ds(target, size), :] = a
        low[pl.ds(target, size), :] = b

    for dy, offset in OFF1.items():
        owner_y = lax.rem(y + dy, NY)

        @pl.loop(0, NZ)
        def _(dz):
            owner_z = lax.rem(z + dz, NZ)
            piece(owner_y * H1 + owner_z * R1, offset + dz * R1, R1)

    for dz, offset in OFF2.items():
        owner_z = lax.rem(z + dz, NZ)

        @pl.loop(0, NY)
        def _(dy):
            owner_y = lax.rem(y + dy, NY)
            piece(BASE2 + owner_z * H2 + owner_y * R2, offset + dy * R2, R2)


def multiply_rows(high, low, first, last, p, out):
    step = 128
    for start in range(first, last, step):
        size = min(step, last - start)
        a = (high[start : start + size, :], low[start : start + size, :])
        out[start - first : start - first + size, :] = dot3(a, p, NT)


def first_product_kernel(idx, mine, other, high, low, out, p_high, p_low):
    x, core = idx[0], idx[1]
    for dc, source in enumerate((mine, other)):
        owner_core = lax.rem(core + dc, NC)
        for dx in range(NX):
            owner = lax.rem(x + dx, NX) * NC + owner_core
            a, b = halves(source[dx * 64 : dx * 64 + 64, :])
            target = pl.ds(pl.multiple_of(owner * 64, 64), 64)
            p_high[target, :] = a
            p_low[target, :] = b
    multiply_rows(high, low, 0, FIRST, (p_high[...], p_low[...]), out)


def second_product_kernel(p_high, p_low, high, low, out):
    multiply_rows(high, low, FIRST, ROWS, (p_high[...], p_low[...]), out)


def inverse_kernel(u_ref, out):
    size = 128
    row = lax.broadcasted_iota(jnp.int32, (size, size), 0)
    col = lax.broadcasted_iota(jnp.int32, (size, size), 1)
    eye = jnp.where(row == col, 1.0, 0.0)
    tiles = BLK // size
    scale_rows, scale_cols, n_tiles, inv = [], [], [], []
    for t in range(tiles):
        u = u_ref[t * size : (t + 1) * size, t * size : (t + 1) * size]
        diagonal = jnp.where(row == col, u, 0.0)
        scale_rows.append(1.0 / jnp.sum(diagonal, axis=1, keepdims=True))
        scale_cols.append(1.0 / jnp.sum(diagonal, axis=0, keepdims=True))
        n_tiles.append(jnp.where(row < col, u, 0.0) * scale_rows[t])
    base = 16
    power = [jnp.where((row // base) == (col // base), n, 0.0) for n in n_tiles]
    inv = [eye - n for n in power]
    for _ in range(3):
        power = [dot_full(n, n) for n in power]
        inv = [v + dot_full(v, n) for v, n in zip(inv, power)]
    while base < size:
        pair = ((row // (2 * base)) == (col // (2 * base))) & ((row // base) != (col // base))
        edge = [jnp.where(pair, n, 0.0) for n in n_tiles]
        left = [dot_full(v, e) for v, e in zip(inv, edge)]
        inv = [v - dot_full(l, v) for v, l in zip(inv, left)]
        base *= 2
    inv = [v * s for v, s in zip(inv, scale_cols)]
    out[...] = jnp.zeros_like(out)
    for t in range(tiles):
        out[t * size : (t + 1) * size, t * size : (t + 1) * size] = inv[t]
    base = size
    while base < BLK:
        for start in range(0, BLK, 2 * base):
            a = slice(start, start + base)
            b = slice(start + base, start + 2 * base)
            left = dot_full(out[a, a], u_ref[a, b])
            out[a, b] = -dot_full(left, out[b, b])
        base *= 2


def scale_kernel(u_inv, a0, a1, a2, b0, b1, b2, out1, out2):
    right = u_inv[...]
    out1[...] = -dot_full(a0[...] + a1[...] + a2[...], right, NT)
    out2[...] = -dot_full(b0[...] + b1[...] + b2[...], right, NT)


def early_update_kernel(*refs):
    chunks, (high, low, out) = refs[:10], refs[10:]
    offsets = [OFF1[0], OFF1[1], OFF1[3]] + [OFF2[d] for d in (0, 1, 7, 2, 6, 3, 5)]
    for k, (chunk, offset) in enumerate(zip(chunks, offsets)):
        rows = chunk.shape[0]
        w = (high[offset : offset + rows, :], low[offset : offset + rows, :])
        term = dot3(halves(chunk[...]), w, TN)
        out[...] = term if k == 0 else out[...] + term


def late_update_kernel(idx, total, a0, a1, b0, b1, high, low, out):
    x, core = idx[0], idx[1]
    one = jnp.concatenate([a0[...], a1[...], b0[...], b1[...]], axis=0)
    value = total[...] + dot3(halves(one), (high[0:FIRST, :], low[0:FIRST, :]), TN)
    for owner_x in range(NX):
        for owner_core in range(NC):
            k = owner_x * NC + owner_core
            dx = lax.rem(owner_x - x + NX, NX)
            dc = lax.rem(owner_core - core + NC, NC)
            target = pl.ds(pl.multiple_of((dc * NX + dx) * 64, 64), 64)
            out[target, :] = value[k * 64 : k * 64 + 64, :]


def columns_kernel(idx, *refs):
    ones, twos, out, held = refs[:5], refs[5:14], refs[14], refs[15]
    z, y = idx[2], idx[3]
    column = z * NY + y
    lanes = pl.ds(pl.multiple_of((column // 8) * 128, 128), 128)
    turn = lax.rem(128 - lax.rem(column, 8) * 16, 128)

    def take(source, start, target, size):
        value = source[pl.ds(start, size), lanes]
        held[pl.ds(pl.multiple_of(target, 8), size), :] = pltpu.roll(value, turn, 1)

    half = H1 // 2
    for dy, parts in ((0, (ones[0],)), (1, (ones[1],)), (3, (ones[2],)), (2, (ones[3], ones[4]))):
        owner_y = lax.rem(y + dy, NY)
        for dz in range(NZ):
            owner_z = lax.rem(z + dz, NZ)
            start = dz * R1
            source = parts[0]
            if len(parts) == 2 and start >= half:
                source, start = parts[1], start - half
            take(source, start, owner_y * H1 + owner_z * R1, R1)
    half = H2 // 2
    order = (0, 1, 7, 2, 6, 3, 5, 4)
    for k, dz in enumerate(order):
        owner_z = lax.rem(z + dz, NZ)
        for dy in range(NY):
            owner_y = lax.rem(y + dy, NY)
            start = dy * R2
            source = twos[k]
            if dz == 4 and start >= half:
                source, start = twos[8], start - half
            take(source, start, BASE2 + owner_z * H2 + owner_y * R2, R2)
    out[...] = held[...].T[:16, :]


def ring(axis):
    n = lax.axis_size(axis)
    right = [(i, (i + 1) % n) for i in range(n)]
    left = [(i, (i - 1) % n) for i in range(n)]
    return n, lambda v: lax.ppermute(v, axis, right), lambda v: lax.ppermute(v, axis, left)


def sum_to_owner(chunks, axis):
    n, right, left = ring(axis)
    far = chunks[n // 2]
    half = far.shape[0] // 2
    a, b = right(far[:half]), left(far[half:])
    for hop in range(n // 2 - 1, 0, -1):
        up, down = chunks[hop], chunks[n - hop]
        if hop == n // 2 - 1:
            up = jnp.concatenate([up[:half] + a, up[half:]], axis=0)
            down = jnp.concatenate([down[:half], down[half:] + b], axis=0)
        else:
            up, down = up + a, down + b
        a, b = right(up), left(down)
    return chunks[0], a, b


def gather(own, axis):
    n, right, left = ring(axis)
    half = own.shape[0] // 2
    chunks = {0: own}
    a = b = own
    for hop in range(1, n // 2):
        a, b = right(a), left(b)
        chunks[n - hop], chunks[hop] = a, b
    return chunks, right(a[:half]), left(b[half:])


def joined(chunks, n, lower, upper):
    parts = []
    for hop in range(n):
        parts += [lower, upper] if hop == n // 2 else [chunks[hop]]
    return jnp.concatenate(parts, axis=0)


def body(diag_block, panel_below, trail_inverse):
    f32, bf16 = jnp.float32, jnp.bfloat16
    shape = jax.ShapeDtypeStruct
    idx = jnp.stack([lax.axis_index(a) for a in ("x", "core", "z", "y")]).astype(jnp.int32)
    swap = lambda v: lax.ppermute(v, "core", [(0, 1), (1, 0)])

    piece = panel_below.T
    near, lower, upper = gather(piece, "x")
    mine = joined(near, NX, lower, upper)
    other = swap(mine)

    part = diag_block.T
    copies = jnp.broadcast_to(part, (NCOL, *part.shape))
    block = lax.all_to_all(copies, COL, split_axis=0, concat_axis=0, tiled=True)
    u_inv = call(inverse_kernel, shape((BLK, BLK), f32), 1, 10**9, smem=False)(
        block.reshape(BLK, BLK)
    )

    high, low = call(prepare_kernel, [shape((ROWS, BLK), bf16)] * 2, 1, 10**8)(idx, trail_inverse)
    early, p_high, p_low = call(
        first_product_kernel,
        [shape((FIRST, BLK), f32), shape((BLK, BLK), bf16), shape((BLK, BLK), bf16)],
        4,
        6 * FIRST * BLK * BLK,
    )(idx, mine, other, high, low)
    later = call(
        second_product_kernel, shape((ROWS - FIRST, BLK), f32), 4, 6 * (ROWS - FIRST) * BLK * BLK, smem=False
    )(p_high, p_low, high, low)

    def partial(offset, rows):
        if offset < FIRST:
            return early[offset : offset + rows]
        return later[offset - FIRST : offset - FIRST + rows]

    ones = {d: partial(OFF1[d], H1) for d in range(NY)}
    twos = {d: partial(OFF2[d], H2) for d in range(NZ)}
    a = sum(sum_to_owner(ones, "y"))
    b = sum(sum_to_owner(twos, "z"))
    a = sum_to_owner({d: a[d * R1 : (d + 1) * R1] for d in range(NZ)}, "z")
    b = sum_to_owner({d: b[d * R2 : (d + 1) * R2] for d in range(NY)}, "y")
    a, b = call(
        scale_kernel, [shape((R1, BLK), f32), shape((R2, BLK), f32)], 7, 12 * 64 * BLK * BLK, smem=False
    )(u_inv, *a, *b)

    a = joined_gather(a, "z")
    b = joined_gather(b, "y")
    ones, a_low, a_up = gather(a, "y")
    twos, b_low, b_up = gather(b, "z")
    order = (0, 1, 7, 2, 6, 3, 5)
    near_ones = [ones[0], ones[1], ones[3]]
    near_twos = [twos[d] for d in order]
    total = call(
        early_update_kernel, shape((BLK, BLK), f32), 12, 6 * (ROWS - FIRST) * BLK * BLK, smem=False
    )(*near_ones, *near_twos, high, low)
    update = call(late_update_kernel, shape((BLK, BLK), f32), 7, 6 * FIRST * BLK * BLK)(
        idx, total, a_low, a_up, b_low, b_up, high, low
    )
    columns = call(
        columns_kernel, shape((16, ROWS), f32), 14, 10**7, scratch=[pltpu.VMEM((ROWS, 128), f32)]
    )(idx, *near_ones, a_low, a_up, *near_twos, b_low, b_up)

    half = NX * 64
    rows = update[:half] + swap(update[half:])
    product = sum(sum_to_owner({d: rows[d * 64 : (d + 1) * 64] for d in range(NX)}, "x"))
    return columns.T, product.T


def joined_gather(own, axis):
    chunks, lower, upper = gather(own, axis)
    return joined(chunks, lax.axis_size(axis), lower, upper)


def solution(mesh):
    torus = Mesh(mesh.devices.reshape(NX, NC, NZ, NY), ("x", "core", "z", "y"))
    return jax.shard_map(
        body,
        mesh=torus,
        in_specs=(P(None, COL), P(COL, ROW), P(ROW, COL)),
        out_specs=(P(ROW, COL), P(COL, ROW)),
        check_vma=False,
    )
```

```python
import jax
import jax.numpy as jnp
from jax import lax
from jax.experimental import pallas as pl
from jax.experimental.pallas import tpu as pltpu
from jax.sharding import Mesh
from jax.sharding import PartitionSpec as P


ROW = ("x", "core")
COL = ("z", "y")
NX, NC, NZ, NY = 4, 2, 8, 4
NR, NCOL = NX * NC, NZ * NY
BLK = 512
ROWS = 2048
PIECE = ROWS // NCOL
CHUNK = NZ * PIECE

ORDER = (2, 1, 3, 0)
OFFSET = {dy: CHUNK * place for place, dy in enumerate(ORDER)}


VMEM = pl.BlockSpec(memory_space=pltpu.VMEM)
SMEM = pl.BlockSpec(memory_space=pltpu.SMEM)
NT = (((1,), (1,)), ((), ()))
TN = (((0,), (0,)), ((), ()))
NN = (((1,), (0,)), ((), ()))


def call(kernel, out, n_in, flops=0, scratch=(), smem=True):
    many = isinstance(out, (list, tuple))
    return pl.pallas_call(
        kernel,
        out_shape=out,
        in_specs=([SMEM] if smem else []) + [VMEM] * n_in,
        out_specs=[VMEM] * len(out) if many else VMEM,
        scratch_shapes=list(scratch),
        cost_estimate=pl.CostEstimate(flops=flops, bytes_accessed=1 << 20, transcendentals=0),
    )


def dot_full(a, b, dims=NN):
    return lax.dot_general(
        a, b, dims, precision=lax.Precision.HIGHEST, preferred_element_type=jnp.float32
    )


def prepare_kernel(idx, w, out):
    x, core, z, y = idx[0], idx[1], idx[2], idx[3]
    shift = (x * NC + core) - (z * NY + y)

    def piece(source, target, size):
        source = pl.multiple_of(source, size)
        target = pl.multiple_of(target, size)
        delta = (source >> 9) * NR + shift
        rows = pl.ds(source, size)
        place = pl.ds(target, size)

        @pl.when(delta > 0)
        def _():
            out[place, :] = w[rows, :]

        @pl.when(delta < 0)
        def _():
            out[place, :] = jnp.zeros((size, BLK), jnp.float32)

        @pl.when(delta == 0)
        def _():
            row = lax.broadcasted_iota(jnp.int32, (size, BLK), 0) + (source & (BLK - 1))
            col = lax.broadcasted_iota(jnp.int32, (size, BLK), 1)
            lower = jnp.where(row >= col, w[rows, :], 0.0)
            out[place, :] = lower + jnp.where(row == col, 1.0, 0.0)

    for dy, offset in OFFSET.items():
        owner_y = lax.rem(y + dy, NY)

        @pl.loop(0, NZ)
        def _(dz):
            owner_z = lax.rem(z + dz, NZ)
            piece(owner_y * CHUNK + owner_z * PIECE, offset + dz * PIECE, PIECE)


def inverse_kernel(idx, u_ref, out, work):
    x, core = idx[0], idx[1]
    size = 128
    row = lax.broadcasted_iota(jnp.int32, (size, size), 0)
    col = lax.broadcasted_iota(jnp.int32, (size, size), 1)
    eye = jnp.where(row == col, 1.0, 0.0)
    tiles = BLK // size
    scale_rows, scale_cols, n_tiles, inv = [], [], [], []
    for t in range(tiles):
        u = u_ref[t * size : (t + 1) * size, t * size : (t + 1) * size]
        diagonal = jnp.where(row == col, u, 0.0)
        scale_rows.append(1.0 / jnp.sum(diagonal, axis=1, keepdims=True))
        scale_cols.append(1.0 / jnp.sum(diagonal, axis=0, keepdims=True))
        n_tiles.append(jnp.where(row < col, u, 0.0) * scale_rows[t])
    base = 16
    power = [jnp.where((row // base) == (col // base), n, 0.0) for n in n_tiles]
    inv = [eye - n for n in power]
    for _ in range(3):
        power = [dot_full(n, n) for n in power]
        inv = [v + dot_full(v, n) for v, n in zip(inv, power)]
    while base < size:
        pair = ((row // (2 * base)) == (col // (2 * base))) & ((row // base) != (col // base))
        edge = [jnp.where(pair, n, 0.0) for n in n_tiles]
        left = [dot_full(v, e) for v, e in zip(inv, edge)]
        inv = [v - dot_full(l, v) for v, l in zip(inv, left)]
        base *= 2
    inv = [v * s for v, s in zip(inv, scale_cols)]
    work[...] = jnp.zeros_like(work)
    for t in range(tiles):
        work[t * size : (t + 1) * size, t * size : (t + 1) * size] = inv[t]
    base = size
    while base < BLK:
        for start in range(0, BLK, 2 * base):
            a = slice(start, start + base)
            b = slice(start + base, start + 2 * base)
            left = dot_full(work[a, a], u_ref[a, b])
            work[a, b] = -dot_full(left, work[b, b])
        base *= 2
    for r in range(tiles):
        place_r = pl.multiple_of(lax.rem(r - x + tiles, tiles) * size, size)
        for c in range(tiles):
            place_c = pl.multiple_of(lax.rem(c - x + tiles, tiles) * size, size)
            block = work[c * size : (c + 1) * size, r * size : (r + 1) * size].T
            block = pltpu.roll(pltpu.roll(block, core * 64, 0), core * 64, 1)
            out[pl.ds(place_r, size), pl.ds(place_c, size)] = block


def scale_kernel(x11, a0, a1, a2, out):
    out[...] = -dot_full(a0[...] + a1[...] + a2[...], x11[...])


def columns_kernel(idx, far_low, far_up, up, down, own, out, held):
    x, core, z, y = idx[0], idx[1], idx[2], idx[3]
    column = z * NY + y
    tile = lax.rem((column >> 3) - x + NX, NX)
    inside = ((((column >> 2) & 1) + core) & 1) * 64 + (column & 3) * 16
    lanes = pl.ds(pl.multiple_of(tile * 128, 128), 128)
    turn = lax.rem(128 - inside, 128)
    half = CHUNK // 2
    for dy, source, first, size in (
        (2, far_low, 0, half), (2, far_up, half, half), (1, up, 0, CHUNK), (3, down, 0, CHUNK), (0, own, 0, CHUNK)
    ):
        owner_y = lax.rem(y + dy, NY)

        @pl.loop(0, size // PIECE)
        def _(k):
            owner_z = lax.rem(z + k + first // PIECE, NZ)
            start = pl.multiple_of(k * PIECE, PIECE)
            target = pl.multiple_of(owner_y * CHUNK + owner_z * PIECE, PIECE)
            value = source[pl.ds(start, PIECE), lanes]
            held[pl.ds(target, PIECE), :] = pltpu.roll(value, turn, 1)

    out[...] = held[...].T[:16, :]


def ring(axis):
    n = lax.axis_size(axis)
    right = [(i, (i + 1) % n) for i in range(n)]
    left = [(i, (i - 1) % n) for i in range(n)]
    return n, lambda v: lax.ppermute(v, axis, right), lambda v: lax.ppermute(v, axis, left)


def sum_to_owner(chunks, axis):
    n, right, left = ring(axis)
    far = chunks[n // 2]
    half = far.shape[0] // 2
    a, b = right(far[:half]), left(far[half:])
    for hop in range(n // 2 - 1, 0, -1):
        up, down = chunks[hop], chunks[n - hop]
        if hop == n // 2 - 1:
            up = jnp.concatenate([up[:half] + a, up[half:]], axis=0)
            down = jnp.concatenate([down[:half], down[half:] + b], axis=0)
        else:
            up, down = up + a, down + b
        a, b = right(up), left(down)
    return chunks[0], a, b


def gather(own, axis):
    n, right, left = ring(axis)
    half = own.shape[0] // 2
    chunks = {0: own}
    a = b = own
    for hop in range(1, n // 2):
        a, b = right(a), left(b)
        chunks[n - hop], chunks[hop] = a, b
    return chunks, right(a[:half]), left(b[half:])


def joined(chunks, n, lower, upper):
    parts = []
    for hop in range(n):
        parts += [lower, upper] if hop == n // 2 else [chunks[hop]]
    return jnp.concatenate(parts, axis=0)


def dot_high(a, b, dims):
    return lax.dot_general(
        a, b, dims, precision=lax.Precision.HIGH, preferred_element_type=jnp.float32
    )


def steps(diag_block, panel_below, trail_inverse):
    f32 = jnp.float32
    shape = jax.ShapeDtypeStruct
    idx = jnp.stack([lax.axis_index(a) for a in ("x", "core", "z", "y")]).astype(jnp.int32)
    swap = lambda v: lax.ppermute(v, "core", [(0, 1), (1, 0)])

    near, lower, upper = gather(panel_below.T, "x")
    mine = joined(near, NX, lower, upper)
    other = swap(mine)
    panel = jnp.stack([mine.reshape(NX, 64, BLK), other.reshape(NX, 64, BLK)], axis=1)
    panel = panel.reshape(BLK, BLK)

    part = diag_block.T
    copies = jnp.broadcast_to(part, (NCOL, *part.shape))
    block = lax.all_to_all(copies, COL, split_axis=0, concat_axis=0, tiled=True)
    x11 = call(
        inverse_kernel, shape((BLK, BLK), f32), 1, 10**9, scratch=[pltpu.VMEM((BLK, BLK), f32)]
    )(idx, block.reshape(BLK, BLK))

    w = call(prepare_kernel, shape((ROWS, BLK), f32), 1, 10**8)(idx, trail_inverse)
    partial = {ORDER[0]: dot_high(w[:CHUNK], panel, NT)}
    later = dot_high(w[CHUNK:], panel, NT)
    for k, dy in enumerate(ORDER[1:]):
        partial[dy] = later[k * CHUNK : (k + 1) * CHUNK]

    part = sum(sum_to_owner(partial, "y"))
    parts = sum_to_owner({d: part[d * PIECE : (d + 1) * PIECE] for d in range(NZ)}, "z")
    own = call(scale_kernel, shape((PIECE, BLK), f32), 4, 12 * PIECE * BLK * BLK, smem=False)(x11, *parts)
    own = joined_gather(own, "z")
    chunks, far_low, far_up = gather(own, "y")
    near = jnp.concatenate([chunks[dy] for dy in ORDER[1:]], axis=0)
    total = dot_high(near, w[CHUNK:], TN)
    update = total + dot_high(jnp.concatenate([far_low, far_up], axis=0), w[:CHUNK], TN)
    columns = call(
        columns_kernel, shape((16, ROWS), f32), 5, 10**7, scratch=[pltpu.VMEM((ROWS, 128), f32)]
    )(idx, far_low, far_up, chunks[1], chunks[3], own)

    blocks = update.reshape(NX, NC, 64, BLK)
    rows = blocks[:, 0] + swap(blocks[:, 1])
    product = sum(sum_to_owner({d: rows[d] for d in range(NX)}, "x"))
    return columns.T, product.T


def joined_gather(own, axis):
    chunks, lower, upper = gather(own, axis)
    return joined(chunks, lax.axis_size(axis), lower, upper)


def solution(mesh):
    torus = Mesh(mesh.devices.reshape(NX, NC, NZ, NY), ("x", "core", "z", "y"))
    return jax.shard_map(
        steps,
        mesh=torus,
        in_specs=(P(None, COL), P(COL, ROW), P(ROW, COL)),
        out_specs=(P(ROW, COL), P(COL, ROW)),
        check_vma=False,
    )
```

```python
import jax
import jax.numpy as jnp
from jax import lax
from jax.experimental import pallas as pl
from jax.experimental.pallas import tpu as pltpu
from jax.sharding import Mesh
from jax.sharding import PartitionSpec as P


ROW = ("x", "core")
COL = ("z", "y")
NX, NC, NZ, NY = 4, 2, 8, 4
NR, NCOL = NX * NC, NZ * NY
BLK = 512
ROWS = 2048
PIECE = ROWS // NCOL
CHUNK = NZ * PIECE

ORDER = (2, 1, 3, 0)
OFFSET = {dy: CHUNK * place for place, dy in enumerate(ORDER)}


VMEM = pl.BlockSpec(memory_space=pltpu.VMEM)
SMEM = pl.BlockSpec(memory_space=pltpu.SMEM)
NT = (((1,), (1,)), ((), ()))
TN = (((0,), (0,)), ((), ()))
NN = (((1,), (0,)), ((), ()))


def call(kernel, out, n_in, flops=0, scratch=(), smem=True, mib=8):
    many = isinstance(out, (list, tuple))
    return pl.pallas_call(
        kernel,
        out_shape=out,
        in_specs=([SMEM] if smem else []) + [VMEM] * n_in,
        out_specs=[VMEM] * len(out) if many else VMEM,
        scratch_shapes=list(scratch),
        compiler_params=pltpu.CompilerParams(vmem_limit_bytes=mib << 20),
        cost_estimate=pl.CostEstimate(flops=flops, bytes_accessed=1 << 20, transcendentals=0),
    )


def dot_full(a, b, dims=NN):
    return lax.dot_general(
        a, b, dims, precision=lax.Precision.HIGHEST, preferred_element_type=jnp.float32
    )


def prepare_kernel(idx, w, out):
    x, core, z, y = idx[0], idx[1], idx[2], idx[3]
    shift = (x * NC + core) - (z * NY + y)

    def piece(source, target, size):
        source = pl.multiple_of(source, size)
        target = pl.multiple_of(target, size)
        delta = (source >> 9) * NR + shift
        rows = pl.ds(source, size)
        place = pl.ds(target, size)

        @pl.when(delta > 0)
        def _():
            out[place, :] = w[rows, :]

        @pl.when(delta < 0)
        def _():
            out[place, :] = jnp.zeros((size, BLK), jnp.float32)

        @pl.when(delta == 0)
        def _():
            row = lax.broadcasted_iota(jnp.int32, (size, BLK), 0) + (source & (BLK - 1))
            col = lax.broadcasted_iota(jnp.int32, (size, BLK), 1)
            lower = jnp.where(row >= col, w[rows, :], 0.0)
            out[place, :] = lower + jnp.where(row == col, 1.0, 0.0)

    for dy, offset in OFFSET.items():
        owner_y = lax.rem(y + dy, NY)

        @pl.loop(0, NZ)
        def _(dz):
            owner_z = lax.rem(z + dz, NZ)
            piece(owner_y * CHUNK + owner_z * PIECE, offset + dz * PIECE, PIECE)


def inverse_kernel(idx, mine, other, out, u, work, left):
    x, core = idx[0], idx[1]
    size = 128
    tiles = BLK // size
    half = BLK // 2
    u[:, pl.ds(pl.multiple_of(core * half, half), half)] = mine[...]
    u[:, pl.ds(pl.multiple_of((1 - core) * half, half), half)] = other[...]
    work[...] = jnp.zeros_like(work)
    row = lax.broadcasted_iota(jnp.int32, (size, size), 0)
    col = lax.broadcasted_iota(jnp.int32, (size, size), 1)
    eye = jnp.where(row == col, 1.0, 0.0)

    def place(t, extent=size):
        return pl.ds(pl.multiple_of(t * size, size), extent)

    @pl.loop(0, tiles // 2)
    def _(k):
        spots = [place(2 * k + t) for t in range(2)]
        parts = [u[spot, spot] for spot in spots]
        diagonals = [jnp.where(row == col, v, 0.0) for v in parts]
        upper = [
            jnp.where(row < col, v, 0.0) / jnp.sum(d, axis=1, keepdims=True)
            for v, d in zip(parts, diagonals)
        ]
        base = 16
        power = [jnp.where((row // base) == (col // base), n, 0.0) for n in upper]
        inv = [eye - n for n in power]
        for _ in range(3):
            power = [dot_full(n, n) for n in power]
            inv = [v + dot_full(v, n) for v, n in zip(inv, power)]
        while base < size:
            pair = ((row // (2 * base)) == (col // (2 * base))) & ((row // base) != (col // base))
            edge = [jnp.where(pair, n, 0.0) for n in upper]
            inv = [v - dot_full(dot_full(v, e), v) for v, e in zip(inv, edge)]
            base *= 2
        for spot, v, d in zip(spots, inv, diagonals):
            work[spot, spot] = v / jnp.sum(d, axis=0, keepdims=True)

    @pl.loop(0, tiles // 2)
    def _(k):
        a, b = place(2 * k), place(2 * k + 1)
        work[a, b] = -dot_full(dot_full(work[a, a], u[a, b]), work[b, b])

    @pl.loop(0, 2)
    def _(k):
        left[:, place(k)] = dot_full(work[:half, :half], u[:half, place(k + 2)])

    @pl.loop(0, 2)
    def _(k):
        work[:half, place(k + 2)] = -dot_full(left[...], work[half:, place(k + 2)])

    @pl.loop(0, tiles * tiles)
    def _(k):
        r, c = k >> 2, k & 3
        block = pltpu.roll(pltpu.roll(work[place(c), place(r)].T, core * 64, 0), core * 64, 1)
        out[place((r - x + tiles) & 3), place((c - x + tiles) & 3)] = block


def scale_kernel(x11, a0, a1, a2, out):
    out[...] = -dot_full(a0[...] + a1[...] + a2[...], x11[...])


def columns_kernel(idx, far_low, far_up, up, down, own, out, held):
    x, core, z, y = idx[0], idx[1], idx[2], idx[3]
    column = z * NY + y
    tile = lax.rem((column >> 3) - x + NX, NX)
    inside = ((((column >> 2) & 1) + core) & 1) * 64 + (column & 3) * 16
    lanes = pl.ds(pl.multiple_of(tile * 128, 128), 128)
    turn = lax.rem(128 - inside, 128)
    half = CHUNK // 2
    for dy, source, first, size in (
        (2, far_low, 0, half), (2, far_up, half, half), (1, up, 0, CHUNK), (3, down, 0, CHUNK), (0, own, 0, CHUNK)
    ):
        owner_y = lax.rem(y + dy, NY)

        @pl.loop(0, size // PIECE)
        def _(k):
            owner_z = lax.rem(z + k + first // PIECE, NZ)
            start = pl.multiple_of(k * PIECE, PIECE)
            target = pl.multiple_of(owner_y * CHUNK + owner_z * PIECE, PIECE)
            value = source[pl.ds(start, PIECE), lanes]
            held[pl.ds(target, PIECE), :] = pltpu.roll(value, turn, 1)

    out[...] = held[...].T[:16, :]


def ring(axis):
    n = lax.axis_size(axis)
    right = [(i, (i + 1) % n) for i in range(n)]
    left = [(i, (i - 1) % n) for i in range(n)]
    return n, lambda v: lax.ppermute(v, axis, right), lambda v: lax.ppermute(v, axis, left)


def shifted(value, axis, hops):
    n = lax.axis_size(axis)
    return lax.ppermute(value, axis, [(i, (i + hops) % n) for i in range(n)])


def sum_to_owner(chunks, axis):
    n, right, left = ring(axis)
    far = chunks[n // 2]
    half = far.shape[0] // 2
    a, b = right(far[:half]), left(far[half:])
    for hop in range(n // 2 - 1, 0, -1):
        up, down = chunks[hop], chunks[n - hop]
        a, b = lax.optimization_barrier((a, b))
        if hop == n // 2 - 1:
            up = jnp.concatenate([up[:half] + a, up[half:]], axis=0)
            down = jnp.concatenate([down[:half], down[half:] + b], axis=0)
        else:
            up, down = up + a, down + b
        a, b = right(up), left(down)
    return chunks[0], a, b


def gather(own, axis):
    n, right, left = ring(axis)
    half = own.shape[0] // 2
    chunks = {0: own}
    a = b = own
    for hop in range(1, n // 2):
        a, b = right(a), left(b)
        chunks[n - hop], chunks[hop] = a, b
    return chunks, right(a[:half]), left(b[half:])


def joined(chunks, n, lower, upper):
    parts = []
    for hop in range(n):
        parts += [lower, upper] if hop == n // 2 else [chunks[hop]]
    return jnp.concatenate(parts, axis=0)


def dot_high(a, b, dims):
    return lax.dot_general(
        a, b, dims, precision=lax.Precision.HIGH, preferred_element_type=jnp.float32
    )


def steps(diag_block, panel_below, trail_inverse):
    f32 = jnp.float32
    shape = jax.ShapeDtypeStruct
    idx = jnp.stack([lax.axis_index(a) for a in ("x", "core", "z", "y")]).astype(jnp.int32)
    swap = lambda v: lax.ppermute(v, "core", [(0, 1), (1, 0)])

    own = panel_below.T
    mine = jnp.stack([own, shifted(own, "x", -1), shifted(own, "x", 2), shifted(own, "x", 1)])
    other = swap(mine)
    panel = jnp.stack([mine, other], axis=1).reshape(BLK, BLK)

    half = BLK // NC
    part = lax.dynamic_slice_in_dim(diag_block.T, lax.axis_index("core") * half, half, 1)
    copies = jnp.broadcast_to(part, (NCOL, *part.shape))
    block = lax.all_to_all(copies, COL, split_axis=0, concat_axis=0, tiled=True).reshape(BLK, half)
    across = swap(block)
    x11 = call(
        inverse_kernel,
        shape((BLK, BLK), f32),
        2,
        10**9,
        scratch=[pltpu.VMEM((BLK, BLK), f32), pltpu.VMEM((BLK, BLK), f32), pltpu.VMEM((half, half), f32)],
    )(idx, block, across)

    w = call(prepare_kernel, shape((ROWS, BLK), f32), 1, 10**8, mib=10)(idx, trail_inverse)
    partial = {ORDER[0]: dot_high(w[:CHUNK], panel, NT)}
    later = dot_high(w[CHUNK:], panel, NT)
    for k, dy in enumerate(ORDER[1:]):
        partial[dy] = later[k * CHUNK : (k + 1) * CHUNK]

    part = sum(sum_to_owner(partial, "y"))
    parts = sum_to_owner({d: part[d * PIECE : (d + 1) * PIECE] for d in range(NZ)}, "z")
    own = call(scale_kernel, shape((PIECE, BLK), f32), 4, 12 * PIECE * BLK * BLK, smem=False)(x11, *parts)
    own = joined_gather(own, "z")
    chunks, far_low, far_up = gather(own, "y")
    near = jnp.concatenate([chunks[dy] for dy in ORDER[1:]], axis=0)
    total = dot_high(near, w[CHUNK:], TN)
    update = total + dot_high(jnp.concatenate([far_low, far_up], axis=0), w[:CHUNK], TN)
    columns = call(
        columns_kernel, shape((16, ROWS), f32), 5, 10**7, scratch=[pltpu.VMEM((ROWS, 128), f32)]
    )(idx, far_low, far_up, chunks[1], chunks[3], own)

    blocks = update.reshape(NX, NC, 64, BLK)
    rows = blocks[:, 0] + swap(blocks[:, 1])
    product = rows[0] + shifted(rows[1], "x", 1) + shifted(rows[3], "x", -1) + shifted(rows[2], "x", 2)
    return columns.T, product.T


def joined_gather(own, axis):
    chunks, lower, upper = gather(own, axis)
    return joined(chunks, lax.axis_size(axis), lower, upper)


def solution(mesh):
    torus = Mesh(mesh.devices.reshape(NX, NC, NZ, NY), ("x", "core", "z", "y"))
    return jax.shard_map(
        steps,
        mesh=torus,
        in_specs=(P(None, COL), P(COL, ROW), P(ROW, COL)),
        out_specs=(P(ROW, COL), P(COL, ROW)),
        check_vma=False,
    )
```

```python
import functools

import jax
import jax.numpy as jnp
from jax import lax
from jax.experimental import pallas as pl
from jax.experimental.pallas import tpu as pltpu
from jax.sharding import Mesh
from jax.sharding import PartitionSpec as P


ROW = ("x", "core")
COL = ("z", "y")
NX, NC, NZ, NY = 4, 2, 8, 4
NR, NCOL = NX * NC, NZ * NY
BLK = 512
ROWS = 2048
PIECE = ROWS // NCOL
CHUNK = NZ * PIECE
WIDTH = 4
TILE = 128
STEP = 256

ORDER = (2, 1, 3, 0)
OFFSET = {dy: CHUNK * place for place, dy in enumerate(ORDER)}


VMEM = pl.BlockSpec(memory_space=pltpu.VMEM)
SMEM = pl.BlockSpec(memory_space=pltpu.SMEM)
NT = (((1,), (1,)), ((), ()))
TN = (((0,), (0,)), ((), ()))
NN = (((1,), (0,)), ((), ()))


def call(kernel, out, n_in, flops=0, scratch=(), smem=True, mib=8):
    many = isinstance(out, (list, tuple))
    return pl.pallas_call(
        kernel,
        out_shape=out,
        in_specs=([SMEM] if smem else []) + [VMEM] * n_in,
        out_specs=[VMEM] * len(out) if many else VMEM,
        scratch_shapes=list(scratch),
        compiler_params=pltpu.CompilerParams(vmem_limit_bytes=mib << 20),
        cost_estimate=pl.CostEstimate(flops=flops, bytes_accessed=1 << 20, transcendentals=0),
    )


def halves(value):
    high = value.astype(jnp.bfloat16)
    low = (value - high.astype(jnp.float32)).astype(jnp.bfloat16)
    return high, low


def dot_full(a, b, dims=NN):
    return lax.dot_general(
        a, b, dims, precision=lax.Precision.HIGHEST, preferred_element_type=jnp.float32
    )


def prepare_kernel(idx, w, out):
    x, core, z, y = idx[0], idx[1], idx[2], idx[3]
    shift = (x * NC + core) - (z * NY + y)

    def piece(source, target, size):
        source = pl.multiple_of(source, size)
        target = pl.multiple_of(target, size)
        delta = (source >> 9) * NR + shift
        rows = pl.ds(source, size)
        place = pl.ds(target, size)

        @pl.when(delta > 0)
        def _():
            out[place, :] = w[rows, :]

        @pl.when(delta < 0)
        def _():
            out[place, :] = jnp.zeros((size, BLK), jnp.float32)

        @pl.when(delta == 0)
        def _():
            row = lax.broadcasted_iota(jnp.int32, (size, BLK), 0) + (source & (BLK - 1))
            col = lax.broadcasted_iota(jnp.int32, (size, BLK), 1)
            lower = jnp.where(row >= col, w[rows, :], 0.0)
            out[place, :] = lower + jnp.where(row == col, 1.0, 0.0)

    for dy, offset in OFFSET.items():
        owner_y = lax.rem(y + dy, NY)

        @pl.loop(0, NZ)
        def _(dz):
            owner_z = lax.rem(z + dz, NZ)
            piece(owner_y * CHUNK + owner_z * PIECE, offset + dz * PIECE, PIECE)


def merge(a, b):
    return dot_three(halves(a), halves(b), NN)


def place(t, extent=TILE):
    return pl.ds(pl.multiple_of(t * TILE, TILE), extent)


def tiles_kernel(idx, mine, other, u, work):
    core = idx[1]
    size = TILE
    tiles = BLK // size
    half = BLK // 2
    u[:, pl.ds(pl.multiple_of(core * half, half), half)] = mine[...]
    u[:, pl.ds(pl.multiple_of((1 - core) * half, half), half)] = other[...]
    work[...] = jnp.zeros_like(work)
    row = lax.broadcasted_iota(jnp.int32, (size, size), 0)
    col = lax.broadcasted_iota(jnp.int32, (size, size), 1)
    eye = jnp.where(row == col, 1.0, 0.0)

    @pl.loop(0, tiles // WIDTH)
    def _(k):
        spots = [place(WIDTH * k + t) for t in range(WIDTH)]
        parts = [u[spot, spot] for spot in spots]
        diagonals = [jnp.where(row == col, v, 0.0) for v in parts]
        upper = [
            jnp.where(row < col, v, 0.0) / jnp.sum(d, axis=1, keepdims=True)
            for v, d in zip(parts, diagonals)
        ]
        base = 16
        power = [jnp.where((row // base) == (col // base), n, 0.0) for n in upper]
        inv = [eye - n for n in power]
        for _ in range(3):
            power = [dot_full(n, n) for n in power]
            inv = [v + dot_full(v, n) for v, n in zip(inv, power)]
        while base < size:
            pair = ((row // (2 * base)) == (col // (2 * base))) & ((row // base) != (col // base))
            edge = [jnp.where(pair, n, 0.0) for n in upper]
            inv = [v - merge(merge(v, e), v) for v, e in zip(inv, edge)]
            base *= 2
        for spot, v, d in zip(spots, inv, diagonals):
            work[spot, spot] = v / jnp.sum(d, axis=0, keepdims=True)


def inverse_kernel(idx, u, diagonal, out, work, left):
    x, core = idx[0], idx[1]
    tiles = BLK // TILE
    half = BLK // 2
    work[...] = diagonal[...]

    @pl.loop(0, tiles // 2)
    def _(k):
        a, b = place(2 * k), place(2 * k + 1)
        work[a, b] = -merge(merge(work[a, a], u[a, b]), work[b, b])

    @pl.loop(0, 2)
    def _(k):
        left[:, place(k)] = merge(work[:half, :half], u[:half, place(k + 2)])

    @pl.loop(0, 2)
    def _(k):
        work[:half, place(k + 2)] = -merge(left[...], work[half:, place(k + 2)])

    @pl.loop(0, tiles * tiles)
    def _(k):
        r, c = k >> 2, k & 3
        block = pltpu.roll(pltpu.roll(work[place(c), place(r)].T, core * 64, 0), core * 64, 1)
        out[place((r - x + tiles) & 3), place((c - x + tiles) & 3)] = block


def halves(value):
    high = value.astype(jnp.bfloat16)
    return high, (value - high.astype(jnp.float32)).astype(jnp.bfloat16)


def dot_three(a, b, dims):
    terms = [
        lax.dot_general(u, v, dims, preferred_element_type=jnp.float32)
        for u, v in ((a[0], b[1]), (a[1], b[0]), (a[0], b[0]))
    ]
    return (terms[0] + terms[1]) + terms[2]


def product_kernel(first, panel, w, *refs):
    outs, high, low = refs[:-2], refs[-2], refs[-1]
    high[...], low[...] = halves(panel[...])
    for out in outs:

        @pl.loop(0, out.shape[0] // STEP)
        def _(i):
            rows = pl.ds(pl.multiple_of(first + i * STEP, STEP), STEP)
            target = pl.ds(pl.multiple_of(i * STEP, STEP), STEP)
            out[target, :] = dot_three(halves(w[rows, :]), (high[...], low[...]), NT)

        first += out.shape[0]


def near_kernel(w, *refs):
    chunks, out = refs[:3], refs[3]
    out[...] = jnp.zeros_like(out)
    for k, chunk in enumerate(chunks):

        @pl.loop(0, CHUNK // STEP)
        def _(i):
            rows = pl.ds(pl.multiple_of(CHUNK * (k + 1) + i * STEP, STEP), STEP)
            source = pl.ds(pl.multiple_of(i * STEP, STEP), STEP)
            out[...] += dot_three(halves(chunk[source, :]), halves(w[rows, :]), TN)


def scale_kernel(x11, a0, a1, a2, out):
    out[...] = -dot_full(a0[...] + a1[...] + a2[...], x11[...])


def columns_kernel(idx, far_low, far_up, up, down, own, out, held):
    x, core, z, y = idx[0], idx[1], idx[2], idx[3]
    column = z * NY + y
    tile = lax.rem((column >> 3) - x + NX, NX)
    inside = ((((column >> 2) & 1) + core) & 1) * 64 + (column & 3) * 16
    lanes = pl.ds(pl.multiple_of(tile * 128, 128), 128)
    turn = lax.rem(128 - inside, 128)
    half = CHUNK // 2
    for dy, source, first, size in (
        (2, far_low, 0, half), (2, far_up, half, half), (1, up, 0, CHUNK), (3, down, 0, CHUNK), (0, own, 0, CHUNK)
    ):
        owner_y = lax.rem(y + dy, NY)

        @pl.loop(0, size // PIECE)
        def _(k):
            owner_z = lax.rem(z + k + first // PIECE, NZ)
            start = pl.multiple_of(k * PIECE, PIECE)
            target = pl.multiple_of(owner_y * CHUNK + owner_z * PIECE, PIECE)
            value = source[pl.ds(start, PIECE), lanes]
            held[pl.ds(target, PIECE), :] = pltpu.roll(value, turn, 1)

    out[...] = held[...].T[:16, :]


def ring(axis):
    n = lax.axis_size(axis)
    right = [(i, (i + 1) % n) for i in range(n)]
    left = [(i, (i - 1) % n) for i in range(n)]
    return n, lambda v: lax.ppermute(v, axis, right), lambda v: lax.ppermute(v, axis, left)


def shifted(value, axis, hops):
    n = lax.axis_size(axis)
    return lax.ppermute(value, axis, [(i, (i + hops) % n) for i in range(n)])


def sum_to_owner(chunks, far, axis):
    n, right, left = ring(axis)
    half = far[0].shape[0]
    a, b = right(far[0]), left(far[1])
    for hop in range(n // 2 - 1, 0, -1):
        a, b = lax.optimization_barrier((a, b))
        if hop == n // 2 - 1:
            a = jnp.pad(a, ((0, half), (0, 0)))
            b = jnp.pad(b, ((half, 0), (0, 0)))
        up, down = chunks[hop] + a, chunks[n - hop] + b
        a, b = right(up), left(down)
    return chunks[0], a, b


def gather(own, axis):
    n, right, left = ring(axis)
    half = own.shape[0] // 2
    chunks = {0: own}
    a = b = own
    for hop in range(1, n // 2):
        a, b = right(a), left(b)
        chunks[n - hop], chunks[hop] = a, b
    return chunks, right(a[:half]), left(b[half:])


def joined(chunks, n, lower, upper):
    parts = []
    for hop in range(n):
        parts += [lower, upper] if hop == n // 2 else [chunks[hop]]
    return jnp.concatenate(parts, axis=0)


def dot_high(a, b, dims):
    return lax.dot_general(
        a, b, dims, precision=lax.Precision.HIGH, preferred_element_type=jnp.float32
    )


def steps(diag_block, panel_below, trail_inverse):
    f32 = jnp.float32
    shape = jax.ShapeDtypeStruct
    idx = jnp.stack([lax.axis_index(a) for a in ("x", "core", "z", "y")]).astype(jnp.int32)
    swap = lambda v: lax.ppermute(v, "core", [(0, 1), (1, 0)])

    own = panel_below.T
    mine = jnp.stack([own, shifted(own, "x", -1), shifted(own, "x", 2), shifted(own, "x", 1)])
    other = swap(mine)
    panel = jnp.stack([mine, other], axis=1).reshape(BLK, BLK)

    half = BLK // NC
    part = lax.dynamic_slice_in_dim(diag_block.T, lax.axis_index("core") * half, half, 1)
    for axis in ("y", "z"):
        copies = jnp.broadcast_to(part, (lax.axis_size(axis), *part.shape))
        part = lax.all_to_all(copies, axis, split_axis=0, concat_axis=0, tiled=True)
        part = part.reshape(-1, half)
    block = part
    across = swap(block)
    square = shape((BLK, BLK), f32)
    u, tiles = call(tiles_kernel, [square] * 2, 2, 10**9)(idx, block, across)
    x11 = call(
        inverse_kernel,
        square,
        2,
        10**9,
        scratch=[pltpu.VMEM((BLK, BLK), f32), pltpu.VMEM((half, half), f32)],
    )(idx, u, tiles)

    w = call(prepare_kernel, shape((ROWS, BLK), f32), 1, 10**8, mib=10)(idx, trail_inverse)

    def product(first, outs):
        rows = sum(out.shape[0] for out in outs)
        return call(
            functools.partial(product_kernel, first),
            outs,
            2,
            6 * rows * BLK * BLK,
            scratch=[pltpu.VMEM((BLK, BLK), jnp.bfloat16)] * 2,
            smem=False,
            mib=14,
        )(panel, w)

    far = product(0, [shape((CHUNK // 2, BLK), f32)] * 2)
    later = product(CHUNK, [shape((CHUNK, BLK), f32)] * 3)
    partial = dict(zip(ORDER[1:], later))

    part = sum(sum_to_owner(partial, far, "y"))
    parts = {d: part[d * PIECE : (d + 1) * PIECE] for d in range(NZ)}
    cut = NZ // 2 * PIECE + PIECE // 2
    far = (part[cut - PIECE // 2 : cut], part[cut : cut + PIECE // 2])
    parts = sum_to_owner(parts, far, "z")
    own = call(scale_kernel, shape((PIECE, BLK), f32), 4, 12 * PIECE * BLK * BLK, smem=False)(x11, *parts)
    own = joined_gather(own, "z")
    chunks, far_low, far_up = gather(own, "y")
    total = call(
        near_kernel, shape((BLK, BLK), f32), 4, 6 * (ROWS - CHUNK) * BLK * BLK, smem=False, mib=14
    )(w, *[chunks[dy] for dy in ORDER[1:]])
    update = total + dot_high(jnp.concatenate([far_low, far_up], axis=0), w[:CHUNK], TN)
    columns = call(
        columns_kernel, shape((16, ROWS), f32), 5, 10**7, scratch=[pltpu.VMEM((ROWS, 128), f32)]
    )(idx, far_low, far_up, chunks[1], chunks[3], own)

    blocks = update.reshape(NX, NC, 64, BLK)
    rows = blocks[:, 0] + swap(blocks[:, 1])
    product = rows[0] + shifted(rows[1], "x", 1) + shifted(rows[3], "x", -1) + shifted(rows[2], "x", 2)
    return columns.T, product.T


def joined_gather(own, axis):
    chunks, lower, upper = gather(own, axis)
    return joined(chunks, lax.axis_size(axis), lower, upper)


def solution(mesh):
    torus = Mesh(mesh.devices.reshape(NX, NC, NZ, NY), ("x", "core", "z", "y"))
    return jax.shard_map(
        steps,
        mesh=torus,
        in_specs=(P(None, COL), P(COL, ROW), P(ROW, COL)),
        out_specs=(P(ROW, COL), P(COL, ROW)),
        check_vma=False,
    )
```

```python
import functools

import jax
import jax.numpy as jnp
from jax import lax
from jax.experimental import pallas as pl
from jax.experimental.pallas import tpu as pltpu
from jax.sharding import Mesh
from jax.sharding import PartitionSpec as P


ROW = ("x", "core")
COL = ("z", "y")
NX, NC, NZ, NY = 4, 2, 8, 4
NR, NCOL = NX * NC, NZ * NY
BLK = 512
ROWS = 2048
PIECE = ROWS // NCOL
HALF = PIECE // 2
CHUNK = NZ * PIECE
WIDTH = 4
TILE = 128
STEP = 256

ORDER = (2, 1, 3, 0)
OFFSET = {dy: CHUNK * place for place, dy in enumerate(ORDER)}


VMEM = pl.BlockSpec(memory_space=pltpu.VMEM)
SMEM = pl.BlockSpec(memory_space=pltpu.SMEM)
NT = (((1,), (1,)), ((), ()))
TN = (((0,), (0,)), ((), ()))
NN = (((1,), (0,)), ((), ()))


def call(kernel, out, n_in, flops=0, scratch=(), smem=True, mib=8, aliases=None):
    many = isinstance(out, (list, tuple))
    return pl.pallas_call(
        kernel,
        out_shape=out,
        in_specs=([SMEM] if smem else []) + [VMEM] * n_in,
        out_specs=[VMEM] * len(out) if many else VMEM,
        scratch_shapes=list(scratch),
        input_output_aliases=aliases or {},
        compiler_params=pltpu.CompilerParams(vmem_limit_bytes=mib << 20),
        cost_estimate=pl.CostEstimate(flops=flops, bytes_accessed=1 << 20, transcendentals=0),
    )


def halves(value):
    high = value.astype(jnp.bfloat16)
    low = (value - high.astype(jnp.float32)).astype(jnp.bfloat16)
    return high, low


def dot_full(a, b, dims=NN):
    return lax.dot_general(
        a, b, dims, precision=lax.Precision.HIGHEST, preferred_element_type=jnp.float32
    )


def prepare_kernel(idx, w, out):
    x, core, z, y = idx[0], idx[1], idx[2], idx[3]
    shift = (x * NC + core) - (z * NY + y)

    def piece(source, target, size):
        source = pl.multiple_of(source, size)
        target = pl.multiple_of(target, size)
        delta = (source >> 9) * NR + shift
        rows = pl.ds(source, size)
        place = pl.ds(target, size)

        @pl.when(delta > 0)
        def _():
            out[place, :] = w[rows, :]

        @pl.when(delta < 0)
        def _():
            out[place, :] = jnp.zeros((size, BLK), jnp.float32)

        @pl.when(delta == 0)
        def _():
            row = lax.broadcasted_iota(jnp.int32, (size, BLK), 0) + (source & (BLK - 1))
            col = lax.broadcasted_iota(jnp.int32, (size, BLK), 1)
            lower = jnp.where(row >= col, w[rows, :], 0.0)
            out[place, :] = lower + jnp.where(row == col, 1.0, 0.0)

    for dy, offset in OFFSET.items():
        for group in range(4):

            @pl.loop(0, NZ // 2)
            def _(k):
                piece(own_rows(z, y, dy, group, k), offset + group * (CHUNK // 4) + k * HALF, HALF)


def own_rows(z, y, dy, group, k):
    parity = z & 1
    first, half = ((1, parity), (7, 1 - parity), (0, 1 - parity), (0, parity))[group]
    return ((y + dy) & (NY - 1)) * CHUNK + ((z + first + 2 * k) & (NZ - 1)) * PIECE + half * HALF


def merge(a, b):
    return dot_three(halves(a), halves(b), NN)


def place(t, extent=TILE):
    return pl.ds(pl.multiple_of(t * TILE, TILE), extent)


def tiles_kernel(idx, mine, other, u, work):
    core = idx[1]
    size = TILE
    tiles = BLK // size
    half = BLK // 2
    u[:, pl.ds(pl.multiple_of(core * half, half), half)] = mine[...]
    u[:, pl.ds(pl.multiple_of((1 - core) * half, half), half)] = other[...]
    work[...] = jnp.zeros_like(work)
    row = lax.broadcasted_iota(jnp.int32, (size, size), 0)
    col = lax.broadcasted_iota(jnp.int32, (size, size), 1)
    eye = jnp.where(row == col, 1.0, 0.0)

    @pl.loop(0, tiles // WIDTH)
    def _(k):
        spots = [place(WIDTH * k + t) for t in range(WIDTH)]
        parts = [u[spot, spot] for spot in spots]
        diagonals = [jnp.where(row == col, v, 0.0) for v in parts]
        upper = [
            jnp.where(row < col, v, 0.0) / jnp.sum(d, axis=1, keepdims=True)
            for v, d in zip(parts, diagonals)
        ]
        base = 16
        power = [jnp.where((row // base) == (col // base), n, 0.0) for n in upper]
        inv = [eye - n for n in power]
        for _ in range(3):
            power = [dot_full(n, n) for n in power]
            inv = [v + dot_full(v, n) for v, n in zip(inv, power)]
        while base < size:
            pair = ((row // (2 * base)) == (col // (2 * base))) & ((row // base) != (col // base))
            edge = [jnp.where(pair, n, 0.0) for n in upper]
            inv = [v - merge(merge(v, e), v) for v, e in zip(inv, edge)]
            base *= 2
        for spot, v, d in zip(spots, inv, diagonals):
            work[spot, spot] = v / jnp.sum(d, axis=0, keepdims=True)


def inverse_kernel(idx, u, diagonal, out, work, left):
    x, core = idx[0], idx[1]
    tiles = BLK // TILE
    half = BLK // 2
    work[...] = diagonal[...]

    @pl.loop(0, tiles // 2)
    def _(k):
        a, b = place(2 * k), place(2 * k + 1)
        work[a, b] = -merge(merge(work[a, a], u[a, b]), work[b, b])

    @pl.loop(0, 2)
    def _(k):
        left[:, place(k)] = merge(work[:half, :half], u[:half, place(k + 2)])

    @pl.loop(0, 2)
    def _(k):
        work[:half, place(k + 2)] = -merge(left[...], work[half:, place(k + 2)])

    @pl.loop(0, tiles * tiles)
    def _(k):
        r, c = k >> 2, k & 3
        block = pltpu.roll(pltpu.roll(work[place(c), place(r)].T, core * 64, 0), core * 64, 1)
        out[place((r - x + tiles) & 3), place((c - x + tiles) & 3)] = block


def halves(value):
    high = value.astype(jnp.bfloat16)
    return high, (value - high.astype(jnp.float32)).astype(jnp.bfloat16)


def dot_three(a, b, dims):
    terms = [
        lax.dot_general(u, v, dims, preferred_element_type=jnp.float32)
        for u, v in ((a[0], b[1]), (a[1], b[0]), (a[0], b[0]))
    ]
    return (terms[0] + terms[1]) + terms[2]


def product_kernel(first, panel, w, *refs):
    outs, high, low = refs[:-2], refs[-2], refs[-1]
    high[...], low[...] = halves(panel[...])
    for out in outs:

        @pl.loop(0, out.shape[0] // STEP)
        def _(i):
            rows = pl.ds(pl.multiple_of(first + i * STEP, STEP), STEP)
            target = pl.ds(pl.multiple_of(i * STEP, STEP), STEP)
            out[target, :] = dot_three(halves(w[rows, :]), (high[...], low[...]), NT)

        first += out.shape[0]


def near_kernel(w, *refs):
    chunks, out = refs[:3], refs[3]
    out[...] = jnp.zeros_like(out)
    for k, chunk in enumerate(chunks):

        @pl.loop(0, CHUNK // STEP)
        def _(i):
            rows = pl.ds(pl.multiple_of(CHUNK * (k + 1) + i * STEP, STEP), STEP)
            source = pl.ds(pl.multiple_of(i * STEP, STEP), STEP)
            out[...] += dot_three(halves(chunk[source, :]), halves(w[rows, :]), TN)


def scale_kernel(x11, a0, a1, a2, out):
    out[...] = -dot_full(a0[...] + a1[...] + a2[...], x11[...])


def take_columns(idx, dys, sources, held):
    x, core, z, y = idx[0], idx[1], idx[2], idx[3]
    column = z * NY + y
    tile = lax.rem((column >> 3) - x + NX, NX)
    inside = ((((column >> 2) & 1) + core) & 1) * 64 + (column & 3) * 16
    lanes = pl.ds(pl.multiple_of(tile * 128, 128), 128)
    turn = lax.rem(128 - inside, 128)
    for dy, parts in zip(dys, sources):
        base = ((y + dy) & (NY - 1)) * CHUNK
        for group in range(4):
            source = parts[group * len(parts) // 4]
            first = group % (4 // len(parts)) * (CHUNK // 4)

            @pl.loop(0, NZ // 2)
            def _(k):
                start = pl.multiple_of(first + k * HALF, HALF)
                target = pl.multiple_of(own_rows(z, y, dy, group, k) - base, HALF)
                value = source[pl.ds(start, HALF), lanes]
                held[pl.ds(target, HALF), :] = pltpu.roll(value, turn, 1)

        yield pl.ds(pl.multiple_of(base, CHUNK), CHUNK), held[...].T[:16, :]


def near_columns_kernel(idx, up, down, own, out, held):
    out[...] = jnp.zeros_like(out)
    for place, value in take_columns(idx, ORDER[1:], ((up,), (down,), (own,)), held):
        out[:, place] = value


def far_columns_kernel(idx, near, low, up, out, held):
    out[...] = near[...]
    for place, value in take_columns(idx, ORDER[:1], ((low, up),), held):
        out[:, place] = value


def ring(axis, stride=1):
    n = lax.axis_size(axis)
    right = [(i, (i + stride) % n) for i in range(n)]
    left = [(i, (i - stride) % n) for i in range(n)]
    return lambda v: lax.ppermute(v, axis, right), lambda v: lax.ppermute(v, axis, left)


def shifted(value, axis, hops):
    n = lax.axis_size(axis)
    return lax.ppermute(value, axis, [(i, (i + hops) % n) for i in range(n)])


def sum_of_four(chunks, far, axis, stride=1):
    right, left = ring(axis, stride)
    a, b = right(far[0]), left(far[1])
    rows = jax.ShapeDtypeStruct(chunks[1].shape, jnp.float32)
    up, down = call(middle_kernel, [rows] * 2, 4, 10**6, smem=False, aliases={0: 0, 1: 1})(
        chunks[1], chunks[3], a, b
    )
    return chunks[0], right(up), left(down)


def middle_kernel(up, down, a, b, up_out, down_out):
    half = a.shape[0]
    up_out[:half, :] = up[:half, :] + a[...]
    down_out[half:, :] = down[half:, :] + b[...]


def gather_of_four(own, axis, stride=1):
    right, left = ring(axis, stride)
    half = own.shape[0] // 2
    a, b = right(own), left(own)
    return {0: own, 1: b, 3: a}, right(a[:half]), left(b[half:])


def dot_high(a, b, dims):
    return lax.dot_general(
        a, b, dims, precision=lax.Precision.HIGH, preferred_element_type=jnp.float32
    )


def steps(diag_block, panel_below, trail_inverse):
    f32 = jnp.float32
    shape = jax.ShapeDtypeStruct
    idx = jnp.stack([lax.axis_index(a) for a in ("x", "core", "z", "y")]).astype(jnp.int32)
    swap = lambda v: lax.ppermute(v, "core", [(0, 1), (1, 0)])

    own = panel_below.T
    mine = jnp.stack([own, shifted(own, "x", -1), shifted(own, "x", 2), shifted(own, "x", 1)])
    other = swap(mine)
    panel = jnp.stack([mine, other], axis=1).reshape(BLK, BLK)

    half = BLK // NC
    part = lax.dynamic_slice_in_dim(diag_block.T, lax.axis_index("core") * half, half, 1)
    for axis in ("y", "z"):
        copies = jnp.broadcast_to(part, (lax.axis_size(axis), *part.shape))
        part = lax.all_to_all(copies, axis, split_axis=0, concat_axis=0, tiled=True)
        part = part.reshape(-1, half)
    block = part
    across = swap(block)
    square = shape((BLK, BLK), f32)
    u, tiles = call(tiles_kernel, [square] * 2, 2, 10**9)(idx, block, across)
    x11 = call(
        inverse_kernel,
        square,
        2,
        10**9,
        scratch=[pltpu.VMEM((BLK, BLK), f32), pltpu.VMEM((half, half), f32)],
    )(idx, u, tiles)

    w = call(prepare_kernel, shape((ROWS, BLK), f32), 1, 10**8, mib=10)(idx, trail_inverse)

    def product(first, outs):
        rows = sum(out.shape[0] for out in outs)
        return call(
            functools.partial(product_kernel, first),
            outs,
            2,
            6 * rows * BLK * BLK,
            scratch=[pltpu.VMEM((BLK, BLK), jnp.bfloat16)] * 2,
            smem=False,
            mib=14,
        )(panel, w)

    far = product(0, [shape((CHUNK // 2, BLK), f32)] * 2)
    later = product(CHUNK, [shape((CHUNK, BLK), f32)] * 3)
    partial = dict(zip(ORDER[1:], later))

    part = sum(sum_of_four(partial, far, "y"))
    right, left = ring("z")
    quarter = CHUNK // 4
    a, b = right(part[:quarter]), left(part[quarter : 2 * quarter])
    a, b = lax.optimization_barrier((a, b))
    a = part[2 * quarter : 3 * quarter] + a
    b = part[3 * quarter :] + b
    spots = [slice(k * HALF, (k + 1) * HALF) for k in range(4)]
    pieces = {k: jnp.concatenate([a[spots[k]], b[spots[k]]], axis=0) for k in (0, 1, 3)}
    parts = sum_of_four(pieces, (a[spots[2]], b[spots[2]]), "z", 2)
    own = call(scale_kernel, shape((PIECE, BLK), f32), 4, 12 * PIECE * BLK * BLK, smem=False)(x11, *parts)
    near, low, up = gather_of_four(own, "z", 2)
    a = jnp.concatenate([near[0][:HALF], near[1][:HALF], low, near[3][:HALF]], axis=0)
    b = jnp.concatenate([near[0][HALF:], near[1][HALF:], up, near[3][HALF:]], axis=0)
    own = jnp.concatenate([left(a), right(b), a, b], axis=0)
    chunks, far_low, far_up = gather_of_four(own, "y")
    total = call(
        near_kernel, shape((BLK, BLK), f32), 4, 6 * (ROWS - CHUNK) * BLK * BLK, smem=False, mib=14
    )(w, *[chunks[dy] for dy in ORDER[1:]])
    update = total + dot_high(jnp.concatenate([far_low, far_up], axis=0), w[:CHUNK], TN)
    held = [pltpu.VMEM((CHUNK, 128), f32)]
    strip = shape((16, ROWS), f32)
    columns = call(near_columns_kernel, strip, 3, 10**7, scratch=held)(
        idx, *[chunks[dy] for dy in ORDER[1:]]
    )
    columns = call(far_columns_kernel, strip, 3, 10**7, scratch=held)(idx, columns, far_low, far_up)

    blocks = update.reshape(NX, NC, 64, BLK)
    rows = blocks[:, 0] + swap(blocks[:, 1])
    product = rows[0] + shifted(rows[1], "x", 1) + shifted(rows[3], "x", -1) + shifted(rows[2], "x", 2)
    return columns.T, product.T


def solution(mesh):
    torus = Mesh(mesh.devices.reshape(NX, NC, NZ, NY), ("x", "core", "z", "y"))
    return jax.shard_map(
        steps,
        mesh=torus,
        in_specs=(P(None, COL), P(COL, ROW), P(ROW, COL)),
        out_specs=(P(ROW, COL), P(COL, ROW)),
        check_vma=False,
    )
```

```python
import functools

import jax
import jax.numpy as jnp
from jax import lax
from jax.experimental import pallas as pl
from jax.experimental.pallas import tpu as pltpu
from jax.sharding import Mesh
from jax.sharding import PartitionSpec as P


ROW = ("x", "core")
COL = ("z", "y")
NX, NC, NZ, NY = 4, 2, 8, 4
NR, NCOL = NX * NC, NZ * NY
BLK = 512
ROWS = 2048
PIECE = ROWS // NCOL
HALF = PIECE // 2
CHUNK = NZ * PIECE
WIDTH = 4
TILE = 128
STEP = 256

ORDER = (2, 1, 3, 0)
OFFSET = {dy: CHUNK * place for place, dy in enumerate(ORDER)}


VMEM = pl.BlockSpec(memory_space=pltpu.VMEM)
SMEM = pl.BlockSpec(memory_space=pltpu.SMEM)
NT = (((1,), (1,)), ((), ()))
TN = (((0,), (0,)), ((), ()))
NN = (((1,), (0,)), ((), ()))


def call(kernel, out, n_in, flops=0, scratch=(), smem=True, mib=8, aliases=None):
    many = isinstance(out, (list, tuple))
    return pl.pallas_call(
        kernel,
        out_shape=out,
        in_specs=([SMEM] if smem else []) + [VMEM] * n_in,
        out_specs=[VMEM] * len(out) if many else VMEM,
        scratch_shapes=list(scratch),
        input_output_aliases=aliases or {},
        compiler_params=pltpu.CompilerParams(vmem_limit_bytes=mib << 20),
        cost_estimate=pl.CostEstimate(flops=flops, bytes_accessed=1 << 20, transcendentals=0),
    )


def halves(value):
    high = value.astype(jnp.bfloat16)
    low = (value - high.astype(jnp.float32)).astype(jnp.bfloat16)
    return high, low


def dot_full(a, b, dims=NN):
    return lax.dot_general(
        a, b, dims, precision=lax.Precision.HIGHEST, preferred_element_type=jnp.float32
    )


def prepare_kernel(idx, w, out):
    x, core, z, y = idx[0], idx[1], idx[2], idx[3]
    shift = (x * NC + core) - (z * NY + y)

    def piece(source, target, size):
        source = pl.multiple_of(source, size)
        target = pl.multiple_of(target, size)
        delta = (source >> 9) * NR + shift
        rows = pl.ds(source, size)
        place = pl.ds(target, size)

        @pl.when(delta > 0)
        def _():
            out[place, :] = w[rows, :]

        @pl.when(delta < 0)
        def _():
            out[place, :] = jnp.zeros((size, BLK), jnp.float32)

        @pl.when(delta == 0)
        def _():
            row = lax.broadcasted_iota(jnp.int32, (size, BLK), 0) + (source & (BLK - 1))
            col = lax.broadcasted_iota(jnp.int32, (size, BLK), 1)
            lower = jnp.where(row >= col, w[rows, :], 0.0)
            out[place, :] = lower + jnp.where(row == col, 1.0, 0.0)

    for dy, offset in OFFSET.items():
        for group in range(4):

            @pl.loop(0, NZ // 2)
            def _(k):
                piece(own_rows(z, y, dy, group, k), offset + group * (CHUNK // 4) + k * HALF, HALF)


def own_rows(z, y, dy, group, k):
    parity = z & 1
    first, half = ((1, parity), (7, 1 - parity), (0, 1 - parity), (0, parity))[group]
    return ((y + dy) & (NY - 1)) * CHUNK + ((z + first + 2 * k) & (NZ - 1)) * PIECE + half * HALF


def merge(a, b):
    return dot_three(halves(a), halves(b), NN)


def place(t, extent=TILE):
    return pl.ds(pl.multiple_of(t * TILE, TILE), extent)


def tiles_kernel(idx, mine, other, u, work):
    core = idx[1]
    size = TILE
    tiles = BLK // size
    half = BLK // 2
    u[:, pl.ds(pl.multiple_of(core * half, half), half)] = mine[...]
    u[:, pl.ds(pl.multiple_of((1 - core) * half, half), half)] = other[...]
    work[...] = jnp.zeros_like(work)
    row = lax.broadcasted_iota(jnp.int32, (size, size), 0)
    col = lax.broadcasted_iota(jnp.int32, (size, size), 1)
    eye = jnp.where(row == col, 1.0, 0.0)

    @pl.loop(0, tiles // WIDTH)
    def _(k):
        spots = [place(WIDTH * k + t) for t in range(WIDTH)]
        parts = [u[spot, spot] for spot in spots]
        diagonals = [jnp.where(row == col, v, 0.0) for v in parts]
        upper = [
            jnp.where(row < col, v, 0.0) / jnp.sum(d, axis=1, keepdims=True)
            for v, d in zip(parts, diagonals)
        ]
        base = 16
        power = [jnp.where((row // base) == (col // base), n, 0.0) for n in upper]
        inv = [eye - n for n in power]
        for _ in range(3):
            power = [dot_full(n, n) for n in power]
            inv = [v + dot_full(v, n) for v, n in zip(inv, power)]
        while base < size:
            pair = ((row // (2 * base)) == (col // (2 * base))) & ((row // base) != (col // base))
            edge = [jnp.where(pair, n, 0.0) for n in upper]
            inv = [v - merge(merge(v, e), v) for v, e in zip(inv, edge)]
            base *= 2
        for spot, v, d in zip(spots, inv, diagonals):
            work[spot, spot] = v / jnp.sum(d, axis=0, keepdims=True)


def inverse_kernel(idx, u, diagonal, out, work, left):
    x, core = idx[0], idx[1]
    tiles = BLK // TILE
    half = BLK // 2
    work[...] = diagonal[...]

    @pl.loop(0, tiles // 2)
    def _(k):
        a, b = place(2 * k), place(2 * k + 1)
        work[a, b] = -merge(merge(work[a, a], u[a, b]), work[b, b])

    @pl.loop(0, 2)
    def _(k):
        left[:, place(k)] = merge(work[:half, :half], u[:half, place(k + 2)])

    @pl.loop(0, 2)
    def _(k):
        work[:half, place(k + 2)] = -merge(left[...], work[half:, place(k + 2)])

    @pl.loop(0, tiles * tiles)
    def _(k):
        r, c = k >> 2, k & 3
        block = pltpu.roll(pltpu.roll(work[place(c), place(r)].T, core * 64, 0), core * 64, 1)
        out[place((r - x + tiles) & 3), place((c - x + tiles) & 3)] = block


def halves(value):
    high = value.astype(jnp.bfloat16)
    return high, (value - high.astype(jnp.float32)).astype(jnp.bfloat16)


def dot_three(a, b, dims):
    terms = [
        lax.dot_general(u, v, dims, preferred_element_type=jnp.float32)
        for u, v in ((a[0], b[1]), (a[1], b[0]), (a[0], b[0]))
    ]
    return (terms[0] + terms[1]) + terms[2]


def product_kernel(first, panel, w, *refs):
    outs, high, low = refs[:-2], refs[-2], refs[-1]
    high[...], low[...] = halves(panel[...])
    for out in outs:

        @pl.loop(0, out.shape[0] // STEP)
        def _(i):
            rows = pl.ds(pl.multiple_of(first + i * STEP, STEP), STEP)
            target = pl.ds(pl.multiple_of(i * STEP, STEP), STEP)
            out[target, :] = dot_three(halves(w[rows, :]), (high[...], low[...]), NT)

        first += out.shape[0]


def near_kernel(w, *refs):
    chunks, out = refs[:-1], refs[-1]
    out[...] = jnp.zeros_like(out)
    for k, chunk in enumerate(chunks):
        first = CHUNK + k * STEP
        out[...] += dot_three(halves(chunk[...]), halves(w[first : first + STEP, :]), TN)


def scale_kernel(x11, a0, a1, a2, out):
    out[...] = -dot_full(a0[...] + a1[...] + a2[...], x11[...])


def take_columns(idx, dys, sources, held):
    x, core, z, y = idx[0], idx[1], idx[2], idx[3]
    column = z * NY + y
    tile = lax.rem((column >> 3) - x + NX, NX)
    inside = ((((column >> 2) & 1) + core) & 1) * 64 + (column & 3) * 16
    lanes = pl.ds(pl.multiple_of(tile * 128, 128), 128)
    turn = lax.rem(128 - inside, 128)
    for dy, parts in zip(dys, sources):
        base = ((y + dy) & (NY - 1)) * CHUNK
        for group in range(4):
            source = parts[group * len(parts) // 4]
            first = group % (4 // len(parts)) * (CHUNK // 4)

            @pl.loop(0, NZ // 2)
            def _(k):
                start = pl.multiple_of(first + k * HALF, HALF)
                target = pl.multiple_of(own_rows(z, y, dy, group, k) - base, HALF)
                value = source[pl.ds(start, HALF), lanes]
                held[pl.ds(target, HALF), :] = pltpu.roll(value, turn, 1)

        yield pl.ds(pl.multiple_of(base, CHUNK), CHUNK), held[...].T[:16, :]


def near_columns_kernel(idx, *refs):
    out, held = refs[6:]
    out[...] = jnp.zeros_like(out)
    for place, value in take_columns(idx, ORDER[1:], (refs[0:2], refs[2:4], refs[4:6]), held):
        out[:, place] = value


def far_columns_kernel(idx, near, low, up, out, held):
    out[...] = near[...]
    for place, value in take_columns(idx, ORDER[:1], ((low, up),), held):
        out[:, place] = value


def ring(axis, stride=1):
    n = lax.axis_size(axis)
    right = [(i, (i + stride) % n) for i in range(n)]
    left = [(i, (i - stride) % n) for i in range(n)]
    return lambda v: lax.ppermute(v, axis, right), lambda v: lax.ppermute(v, axis, left)


def shifted(value, axis, hops):
    n = lax.axis_size(axis)
    return lax.ppermute(value, axis, [(i, (i + hops) % n) for i in range(n)])


def sum_of_four(chunks, far, axis, stride=1):
    right, left = ring(axis, stride)
    a, b = right(far[0]), left(far[1])
    rows = jax.ShapeDtypeStruct(chunks[1].shape, jnp.float32)
    up, down = call(middle_kernel, [rows] * 2, 4, 10**6, smem=False, aliases={0: 0, 1: 1})(
        chunks[1], chunks[3], a, b
    )
    return chunks[0], right(up), left(down)


def middle_kernel(up, down, a, b, up_out, down_out):
    half = a.shape[0]
    up_out[:half, :] = up[:half, :] + a[...]
    down_out[half:, :] = down[half:, :] + b[...]


def gather_of_four(own, axis, stride=1):
    right, left = ring(axis, stride)
    half = own.shape[0] // 2
    a, b = right(own), left(own)
    a, b = lax.optimization_barrier((a, b))
    low, up = right(a[:half]), left(b[half:])
    low, up = lax.optimization_barrier((low, up))
    return {0: own, 1: b, 3: a}, low, up


def dot_high(a, b, dims):
    return lax.dot_general(
        a, b, dims, precision=lax.Precision.HIGH, preferred_element_type=jnp.float32
    )


def steps(diag_block, panel_below, trail_inverse):
    f32 = jnp.float32
    shape = jax.ShapeDtypeStruct
    idx = jnp.stack([lax.axis_index(a) for a in ("x", "core", "z", "y")]).astype(jnp.int32)
    swap = lambda v: lax.ppermute(v, "core", [(0, 1), (1, 0)])

    own = panel_below.T
    mine = jnp.stack([own, shifted(own, "x", -1), shifted(own, "x", 2), shifted(own, "x", 1)])
    other = swap(mine)
    panel = jnp.stack([mine, other], axis=1).reshape(BLK, BLK)

    half = BLK // NC
    part = lax.dynamic_slice_in_dim(diag_block.T, lax.axis_index("core") * half, half, 1)
    for axis in ("y", "z"):
        copies = jnp.broadcast_to(part, (lax.axis_size(axis), *part.shape))
        part = lax.all_to_all(copies, axis, split_axis=0, concat_axis=0, tiled=True)
        part = part.reshape(-1, half)
    block = part
    across = swap(block)
    square = shape((BLK, BLK), f32)
    u, tiles = call(tiles_kernel, [square] * 2, 2, 10**9)(idx, block, across)
    x11 = call(
        inverse_kernel,
        square,
        2,
        10**9,
        scratch=[pltpu.VMEM((BLK, BLK), f32), pltpu.VMEM((half, half), f32)],
    )(idx, u, tiles)

    w = call(prepare_kernel, shape((ROWS, BLK), f32), 1, 10**8, mib=10)(idx, trail_inverse)

    def product(first, outs):
        rows = sum(out.shape[0] for out in outs)
        return call(
            functools.partial(product_kernel, first),
            outs,
            2,
            6 * rows * BLK * BLK,
            scratch=[pltpu.VMEM((BLK, BLK), jnp.bfloat16)] * 2,
            smem=False,
            mib=14,
        )(panel, w)

    far = product(0, [shape((CHUNK // 2, BLK), f32)] * 2)
    later = product(CHUNK, [shape((CHUNK, BLK), f32)] * 3)
    partial = dict(zip(ORDER[1:], later))

    part = sum(sum_of_four(partial, far, "y"))
    right, left = ring("z")
    quarter = CHUNK // 4
    a, b = right(part[:quarter]), left(part[quarter : 2 * quarter])
    a, b = lax.optimization_barrier((a, b))
    a = part[2 * quarter : 3 * quarter] + a
    b = part[3 * quarter :] + b
    spots = [slice(k * HALF, (k + 1) * HALF) for k in range(4)]
    pieces = {k: jnp.concatenate([a[spots[k]], b[spots[k]]], axis=0) for k in (0, 1, 3)}
    parts = sum_of_four(pieces, (a[spots[2]], b[spots[2]]), "z", 2)
    own = call(scale_kernel, shape((PIECE, BLK), f32), 4, 12 * PIECE * BLK * BLK, smem=False)(x11, *parts)
    near, low, up = gather_of_four(own, "z", 2)
    a = jnp.concatenate([near[0][:HALF], near[1][:HALF], low, near[3][:HALF]], axis=0)
    b = jnp.concatenate([near[0][HALF:], near[1][HALF:], up, near[3][HALF:]], axis=0)
    even = jnp.concatenate([a, b], axis=0)
    right_of_y, left_of_y = ring("y")
    down_even, up_even = right_of_y(even), left_of_y(even)
    odd = jnp.concatenate([left(a), right(b)], axis=0)
    down_odd, up_odd = right_of_y(odd), left_of_y(odd)
    far_up, far_low = left_of_y(up_even), right_of_y(down_odd)
    near = [up_odd, up_even, down_odd, down_even, odd, even]
    total = call(
        near_kernel, shape((BLK, BLK), f32), 7, 6 * (ROWS - CHUNK) * BLK * BLK, smem=False, mib=14
    )(w, *near)
    update = total + dot_high(jnp.concatenate([far_low, far_up], axis=0), w[:CHUNK], TN)
    held = [pltpu.VMEM((CHUNK, 128), f32)]
    strip = shape((16, ROWS), f32)
    columns = call(near_columns_kernel, strip, 6, 10**7, scratch=held)(idx, *near)
    columns = call(far_columns_kernel, strip, 3, 10**7, scratch=held)(idx, columns, far_low, far_up)

    blocks = update.reshape(NX, NC, 64, BLK)
    rows = blocks[:, 0] + swap(blocks[:, 1])
    product = rows[0] + shifted(rows[1], "x", 1) + shifted(rows[3], "x", -1) + shifted(rows[2], "x", 2)
    return columns.T, product.T


def solution(mesh):
    torus = Mesh(mesh.devices.reshape(NX, NC, NZ, NY), ("x", "core", "z", "y"))
    return jax.shard_map(
        steps,
        mesh=torus,
        in_specs=(P(None, COL), P(COL, ROW), P(ROW, COL)),
        out_specs=(P(ROW, COL), P(COL, ROW)),
        check_vma=False,
    )
```
